32 devices in a mesh: slab: 8 (over z, x), rhs: 4 (over y, core).
Axes of the slice: x: 2, y: 2, z: 4, core: 2. Of those that a mesh axis runs over, the one named last changes fastest.
Arguments:
- diag_blocks: float32 [8, 512, 512], P('slab'), may hold values from -1 to 2, as said below
- sub_blocks: float32 [8, 512, 512], P('slab'), may hold values from -1 to 1
- right_side: float32 [256, 4096], P('rhs', 'slab'), may hold values from -6 to 6
- boundary: float32 [512, 256], P(None, 'rhs'), may hold values from -6 to 6
Outputs:
- solution: float32 [256, 4096], P('rhs', 'slab')
The draws below stay inside these ranges and needn't reach their ends.
Inputs may be any that keep to these rules, and one draw needn't show every extreme that they name: Each diag_blocks tile is lower triangular with diagonal entries from 0.8 to 1.25; each sub_blocks tile is upper triangular (zeros below its diagonal).
All inputs are finite; a program needn't handle non-finite values.
Results may differ from the reference program's by a relative error of at most 0.00021.
Values sent between devices are 32-bit elements; how exact they have to be, the bound alone decides.
A program may use at most 64 MiB of HBM per device.

```python
import jax
import jax.numpy as jnp
from jax import lax

B = 512
NRHS = 256
TILE_DEV = 1
TILES = 8
ORDER = 4096
N_SLAB = 8


def draw_diag_blocks(key, part):
    first, second = jax.random.split(jax.random.fold_in(key, 11))
    lower_part = jax.random.normal(first, (TILE_DEV * N_SLAB, B, B), jnp.float32) * (0.3 / B ** 0.5)
    diag_vals = jax.random.uniform(second, (TILE_DEV * N_SLAB, B), jnp.float32, 0.8, 1.25)
    return jnp.tril(lower_part, -1) + jnp.eye(B, dtype=jnp.float32)[None, :, :] * diag_vals[:, None, :]


def draw_sub_blocks(key, part):
    base = jax.random.fold_in(key, 23)
    first, second, third, fourth, fifth = jax.random.split(base, 5)
    upper_part = jax.random.normal(first, (TILE_DEV * N_SLAB, B, B), jnp.float32) * (0.1 / B ** 0.5)
    slow_rate = jnp.exp(jnp.log(0.1) * jax.random.uniform(second, (B,), jnp.float32, 0.3, 1.0) / (TILE_DEV * N_SLAB))
    fast_rate = jax.random.uniform(third, (B,), jnp.float32, 0.2, 0.7)
    is_slow = jax.random.bernoulli(fourth, 0.5, (B,))
    signs = jnp.where(jax.random.bernoulli(fifth, 0.5, (B,)), 1.0, -1.0)
    diag_vals = signs * jnp.where(is_slow, slow_rate, fast_rate)
    return jnp.triu(upper_part, 1) + jnp.eye(B, dtype=jnp.float32)[None, :, :] * diag_vals[None, None, :]


def block_levels(rng, extent, shards, smallest, largest):
    def one(axis_at, blocks):
        draws = jax.random.uniform(jax.random.fold_in(jax.random.fold_in(rng, 6), axis_at), (blocks,), jnp.float32, smallest / len(shards), largest / len(shards))
        return jnp.repeat(jnp.exp(draws), extent[axis_at] // blocks).reshape((-1,) + (1,) * (len(extent) - axis_at - 1))

    factor_of = one(*shards[0])
    for cut in shards[1:]:
        factor_of = factor_of * one(*cut)
    return factor_of


def bell_draw(key, shape, spread, limit, shards=(), kind=jnp.bfloat16):
    values = spread * jax.random.normal(key, shape, jnp.float32)
    if shards:
        values = values * block_levels(key, shape, shards, -0.22, 0.18)
    return jnp.clip(values, -limit, limit).astype(kind)


def setup_inputs(seed: int = 0) -> dict:
    key_list = jax.random.split(jax.random.key(seed), 5)
    diag_blocks = draw_diag_blocks(jax.random.fold_in(key_list[4], 71), 0)
    sub_blocks = draw_sub_blocks(jax.random.fold_in(key_list[4], 71), 0)
    right_side = bell_draw(key_list[2], (NRHS, ORDER), 1.0, 6.0, ((0, 4), (1, 8)), jnp.float32)
    boundary = bell_draw(key_list[3], (B, NRHS), 1.0, 6.0, ((1, 4),), jnp.float32)
    return dict(diag_blocks=diag_blocks, sub_blocks=sub_blocks, right_side=right_side, boundary=boundary)


def reference(diag_blocks, sub_blocks, right_side, boundary):
    tiles_rhs = right_side.reshape(NRHS, TILES, B).transpose(1, 2, 0)

    def advance(previous, items):
        lower, upper, rhs_tile = items
        pushed = jnp.dot(upper, previous, precision=lax.Precision.HIGHEST)
        current = jax.scipy.linalg.solve_triangular(lower, rhs_tile - pushed, lower=True)
        return (current, current)
    final, solved = lax.scan(advance, boundary.astype(jnp.float32), (diag_blocks, sub_blocks, tiles_rhs))
    return solved.transpose(2, 0, 1).reshape(NRHS, ORDER)
```

```python
import functools

import jax
import jax.numpy as jnp
from jax import lax
from jax.experimental import pallas as pl
from jax.experimental.pallas import tpu as pltpu
from jax.sharding import PartitionSpec as P

BASE = 128
CHUNKS = 4
MESH = pl.DeviceIdType.MESH
NN = (((1,), (0,)), ((), ()))
NT = (((1,), (1,)), ((), ()))


def split(value):
    high = value.astype(jnp.bfloat16)
    low = (value - high.astype(jnp.float32)).astype(jnp.bfloat16)
    return high, low


def mul(left, right, dims=NN):
    dot = functools.partial(lax.dot_general, dimension_numbers=dims, preferred_element_type=jnp.float32)
    return dot(left[0], right[0]) + (dot(left[0], right[1]) + dot(left[1], right[0]))


def kernel(n, diag_hbm, sub_hbm, right_hbm, bound_hbm, out_hbm,
           diag, sub, right, inverse, norm, inv_hi, inv_lo, subt_hi, subt_lo,
           spike_hi, spike_lo, part, inflow, solved,
           load_sem, send_sem, recv_sem, store_sem):
    me = lax.axis_index("slab")
    width = diag.shape[0]
    columns = right.shape[0]
    rows = columns // CHUNKS
    loads = []
    for k, (src, dst) in enumerate(((diag_hbm.at[0], diag), (sub_hbm.at[0], sub), (right_hbm, right))):
        loads.append(pltpu.make_async_copy(src, dst, load_sem.at[k]))
        loads[-1].start()
    first, last = me == 0, me == n - 1
    seed = pltpu.make_async_copy(bound_hbm, inflow, load_sem.at[3])

    @pl.when(first)
    def _():
        seed.start()

    after, before = lax.rem(me + 1, n), lax.rem(me + n - 1, n)
    barrier = pltpu.get_barrier_semaphore()
    for other in (before, after):
        pl.semaphore_signal(barrier, inc=1, device_id={"slab": other}, device_id_type=MESH)

    row = lax.broadcasted_iota(jnp.int32, (BASE, BASE), 0)
    col = lax.broadcasted_iota(jnp.int32, (BASE, BASE), 1)
    apart = jnp.where(row > col, row ^ col, 0)
    eye = jnp.where(row == col, 1.0, 0.0).astype(jnp.float32)
    loads[0].wait()
    starts = range(0, width, BASE)
    blocks, scales = [], []
    for at in starts:
        tile = diag[at:at + BASE, at:at + BASE]
        only = tile * eye
        scale = 1.0 / jnp.sum(only, axis=1, keepdims=True)
        scales.append(1.0 / jnp.sum(only, axis=0, keepdims=True))
        for left in range(0, at, BASE):
            norm[at:at + BASE, left:left + BASE] = diag[at:at + BASE, left:left + BASE] * scale
        blocks.append(tile * scale)
    found = [eye - jnp.where(apart == 1, block, 0.0) for block in blocks]
    size = 2
    while size < BASE:
        level = (apart >= size) & (apart < 2 * size)
        pairs = [split(x) for x in found]
        lower = [split(jnp.where(level, block, 0.0)) for block in blocks]
        half = [mul(a, b) for a, b in zip(lower, pairs)]
        found = [x - mul(pair, split(h)) for x, pair, h in zip(found, pairs, half)]
        size *= 2
    for at, x in zip(starts, found):
        inverse[at:at + BASE, at:at + BASE] = x
        for over in range(at + BASE, width, BASE):
            inverse[at:at + BASE, over:over + BASE] = jnp.zeros((BASE, BASE), jnp.float32)
    while size < width:
        for at in range(0, width, 2 * size):
            mid, end = at + size, at + 2 * size
            half = mul(split(norm[mid:end, at:mid]), split(inverse[at:mid, at:mid]))
            inverse[mid:end, at:mid] = -mul(split(inverse[mid:end, mid:end]), split(half))
        size *= 2
    for at, scale in zip(starts, scales):
        high, low = split(inverse[:, at:at + BASE] * scale)
        inv_hi[:, at:at + BASE] = high
        inv_lo[:, at:at + BASE] = low

    loads[1].wait()
    high, low = split(sub[...].T)
    subt_hi[...] = high
    subt_lo[...] = low
    cut = width // 2

    def take(pair, rows_at, cols_at):
        return pair[0][rows_at, cols_at], pair[1][rows_at, cols_at]

    subt, inv, spike = (subt_hi, subt_lo), (inv_hi, inv_lo), (spike_hi, spike_lo)
    top, bot, full = slice(0, cut), slice(cut, width), slice(0, width)

    def put(rows_at, cols_at, value):
        high, low = split(value)
        spike_hi[rows_at, cols_at] = high
        spike_lo[rows_at, cols_at] = low

    put(full, top, mul(take(subt, full, top), take(inv, top, top), NT))
    put(top, bot, mul(take(subt, top, top), take(inv, bot, top), NT))
    put(bot, bot, mul(take(subt, bot, full), take(inv, bot, full), NT))
    loads[2].wait()
    given = split(right[...])
    part[:, top] = mul((given[0][:, top], given[1][:, top]), take(inv, top, top), NT)
    part[:, bot] = mul(given, take(inv, bot, full), NT)


    def send(c):
        at = slice(c * rows, (c + 1) * rows)
        return pltpu.make_async_remote_copy(
            src_ref=solved.at[at], dst_ref=inflow.at[at], send_sem=send_sem.at[c], recv_sem=recv_sem.at[c],
            device_id={"slab": after}, device_id_type=MESH)

    def store(c):
        at = slice(c * rows, (c + 1) * rows)
        return pltpu.make_async_copy(solved.at[at], out_hbm.at[at], store_sem.at[c])

    @pl.when(first)
    def _():
        seed.wait()

    pl.semaphore_wait(barrier, 2)
    for c in range(CHUNKS):
        at = slice(c * rows, (c + 1) * rows)

        @pl.when(jnp.logical_not(first))
        def _():
            send(c).wait_recv()

        high, low = split(inflow[at, :])
        dot = functools.partial(jnp.dot, preferred_element_type=jnp.float32)
        both = dot(jnp.concatenate([high, low], axis=0), spike_hi[...])
        solved[at, :] = part[at, :] - (both[:rows] + both[rows:] + dot(high, spike_lo[...]))

        @pl.when(jnp.logical_not(last))
        def _():
            send(c).start()

        store(c).start()
    for c in range(CHUNKS):
        store(c).wait()

        @pl.when(jnp.logical_not(last))
        def _():
            send(c).wait_send()


def solution(mesh):
    n = mesh.shape["slab"]

    def local(diag_blocks, sub_blocks, right_side, boundary):
        width = diag_blocks.shape[1]
        columns = right_side.shape[0]
        square, flat = (width, width), (columns, width)
        f32, bf16 = jnp.float32, jnp.bfloat16
        return pl.pallas_call(
            functools.partial(kernel, n),
            out_shape=jax.ShapeDtypeStruct(right_side.shape, f32),
            in_specs=[pl.BlockSpec(memory_space=pl.ANY)] * 4,
            out_specs=pl.BlockSpec(memory_space=pl.ANY),
            scratch_shapes=[
                pltpu.VMEM(square, f32), pltpu.VMEM(square, f32), pltpu.VMEM(flat, f32),
                pltpu.VMEM(square, f32), pltpu.VMEM(square, f32), pltpu.VMEM(square, bf16), pltpu.VMEM(square, bf16),
                pltpu.VMEM(square, bf16), pltpu.VMEM(square, bf16), pltpu.VMEM(square, bf16), pltpu.VMEM(square, bf16),
                pltpu.VMEM(flat, f32), pltpu.VMEM(flat, f32), pltpu.VMEM(flat, f32),
                pltpu.SemaphoreType.DMA((4,)), pltpu.SemaphoreType.DMA((CHUNKS,)),
                pltpu.SemaphoreType.DMA((CHUNKS,)), pltpu.SemaphoreType.DMA((CHUNKS,)),
            ],
            compiler_params=pltpu.CompilerParams(collective_id=0, has_side_effects=True),
        )(diag_blocks, sub_blocks, right_side, boundary.T)

    in_specs = (P("slab", None, None), P("slab", None, None), P("rhs", "slab"), P(None, "rhs"))
    return jax.shard_map(local, mesh=mesh, in_specs=in_specs, out_specs=P("rhs", "slab"), check_vma=False)
```

```python
import functools

import jax
import jax.numpy as jnp
from jax import lax
from jax.experimental import pallas as pl
from jax.experimental.pallas import tpu as pltpu
from jax.sharding import PartitionSpec as P

BASE = 128
CHUNKS = 4
PIECES = 8
JOIN = 4
MESH = pl.DeviceIdType.MESH
NN = (((1,), (0,)), ((), ()))
NT = (((1,), (1,)), ((), ()))


def split(value):
    high = value.astype(jnp.bfloat16)
    low = (value - high.astype(jnp.float32)).astype(jnp.bfloat16)
    return high, low


def mul(left, right, dims=NN):
    dot = functools.partial(lax.dot_general, dimension_numbers=dims, preferred_element_type=jnp.float32)
    return dot(left[0], right[0]) + (dot(left[0], right[1]) + dot(left[1], right[0]))


def kernel(n, group, diag_hbm, sub_hbm, right_hbm, bound_hbm, out_hbm,
           diag, sub, right, inverse, norm, inv_hi, inv_lo, subt_hi, subt_lo,
           spike_hi, spike_lo, part, inflow, solved, spike, near_part, near_spike, joint,
           load_sem, send_sem, skip_sem, recv_sem, store_sem, lead_send, lead_recv, part_sem,
           core_send, core_recv, side_send, side_recv, relay_send, relay_recv):
    me = lax.axis_index("slab")
    width = diag.shape[0]
    columns = right.shape[0]
    rows = columns // CHUNKS
    loads = []
    for k, (src, dst) in enumerate(((diag_hbm.at[0], diag), (sub_hbm.at[0], sub), (right_hbm, right))):
        loads.append(pltpu.make_async_copy(src, dst, load_sem.at[k]))
        loads[-1].start()
    first, last = me == 0, me == n - 1
    seed = pltpu.make_async_copy(bound_hbm, inflow, load_sem.at[3])

    @pl.when(first)
    def _():
        seed.start()

    paired = group == 4
    seat = lax.axis_index("rhs")
    twin, side = seat + 1 - 2 * lax.rem(seat, 2), seat + 2 - 4 * (seat // 2)
    odd = lax.rem(me, 2) == 1
    far = odd & (me >= JOIN)
    giver = jnp.logical_not(odd) & (me >= JOIN) & (me < n - 1)
    barrier = pltpu.get_barrier_semaphore()
    greet = [(me >= 1, {"slab": me - 1}), (me < n - 1, {"slab": me + 1})]
    if paired:
        greet += [(odd & (me > JOIN), {"slab": me - 2}), (odd & (me >= JOIN - 1) & (me < n - 2), {"slab": me + 2})]
        greet += [(far, {"rhs": twin}), (far, {"rhs": side})]

    for there, target in greet:
        @pl.when(there)
        def _():
            pl.semaphore_signal(barrier, inc=1, device_id=target, device_id_type=MESH)


    row = lax.broadcasted_iota(jnp.int32, (BASE, BASE), 0)
    col = lax.broadcasted_iota(jnp.int32, (BASE, BASE), 1)
    apart = jnp.where(row > col, row ^ col, 0)
    eye = jnp.where(row == col, 1.0, 0.0).astype(jnp.float32)
    loads[0].wait()
    starts = range(0, width, BASE)
    blocks, scales = [], []
    for at in starts:
        tile = diag[at:at + BASE, at:at + BASE]
        only = tile * eye
        scale = 1.0 / jnp.sum(only, axis=1, keepdims=True)
        scales.append(1.0 / jnp.sum(only, axis=0, keepdims=True))
        for left in range(0, at, BASE):
            norm[at:at + BASE, left:left + BASE] = diag[at:at + BASE, left:left + BASE] * scale
        blocks.append(tile * scale)
    found = [eye - jnp.where(apart == 1, block, 0.0) for block in blocks]
    size = 2
    while size < BASE:
        level = (apart >= size) & (apart < 2 * size)
        pairs = [split(x) for x in found]
        lower = [split(jnp.where(level, block, 0.0)) for block in blocks]
        half = [mul(a, b) for a, b in zip(lower, pairs)]
        found = [x - mul(pair, split(h)) for x, pair, h in zip(found, pairs, half)]
        size *= 2
    for at, x in zip(starts, found):
        inverse[at:at + BASE, at:at + BASE] = x
        for over in range(at + BASE, width, BASE):
            inverse[at:at + BASE, over:over + BASE] = jnp.zeros((BASE, BASE), jnp.float32)
    while size < width:
        for at in range(0, width, 2 * size):
            mid, end = at + size, at + 2 * size
            half = mul(split(norm[mid:end, at:mid]), split(inverse[at:mid, at:mid]))
            inverse[mid:end, at:mid] = -mul(split(inverse[mid:end, mid:end]), split(half))
        size *= 2
    for at, scale in zip(starts, scales):
        high, low = split(inverse[:, at:at + BASE] * scale)
        inv_hi[:, at:at + BASE] = high
        inv_lo[:, at:at + BASE] = low

    loads[1].wait()
    high, low = split(sub[...].T)
    subt_hi[...] = high
    subt_lo[...] = low
    cut = width // 2

    def take(pair, rows_at, cols_at):
        return pair[0][rows_at, cols_at], pair[1][rows_at, cols_at]

    subt, inv = (subt_hi, subt_lo), (inv_hi, inv_lo)
    top, bot, full = slice(0, cut), slice(cut, width), slice(0, width)

    loads[2].wait()
    given = split(right[...])
    part[:, top] = mul((given[0][:, top], given[1][:, top]), take(inv, top, top), NT)
    part[:, bot] = mul(given, take(inv, bot, full), NT)
    pl.semaphore_wait(barrier, sum(jnp.where(there, 1, 0) for there, _ in greet))

    def remote(src, dst, out_sem, in_sem, target):
        return pltpu.make_async_remote_copy(
            src_ref=src, dst_ref=dst, send_sem=out_sem, recv_sem=in_sem, device_id=target, device_id_type=MESH)

    if paired:
        share = width // group
        step = share // PIECES

        def strip(of, piece):
            return pl.ds(pl.multiple_of(of * share + piece * step, step), step)

        def lead_part():
            return remote(part, near_part, part_sem.at[0], part_sem.at[1], {"slab": me + 1})

        def lead(p):
            return remote(spike.at[strip(seat, p)], near_spike.at[pl.ds(p * step, step)],
                          lead_send.at[p], lead_recv.at[p], {"slab": me + 1})

        def to_twin(p):
            at = strip(seat, p)
            return remote(joint.at[at], joint.at[at], core_send.at[p], core_recv.at[p], {"rhs": twin})

        def to_side(p):
            at = strip(seat, p)
            return remote(joint.at[at], joint.at[at], side_send.at[p], side_recv.at[p], {"rhs": side})

        def relay(p):
            at = strip(side, p)
            return remote(joint.at[at], joint.at[at], relay_send.at[p], relay_recv.at[p], {"rhs": twin})

    def put(rows_at, cols_at, value):
        high, low = split(value)
        spike_hi[rows_at, cols_at] = high
        spike_lo[rows_at, cols_at] = low

    if paired:
        @pl.when(giver)
        def _():
            own = pl.ds(pl.multiple_of(seat * share, share), share)
            mine = subt_hi[own, :], subt_lo[own, :]
            spike[own, :] = mul(mine, (inv_hi[...], inv_lo[...]), NT)
            for p in range(PIECES):
                lead(p).start()
            lead_part().start()

    put(full, top, mul(take(subt, full, top), take(inv, top, top), NT))
    put(top, bot, mul(take(subt, top, top), take(inv, bot, top), NT))
    put(bot, bot, mul(take(subt, bot, full), take(inv, bot, full), NT))

    if paired:
        @pl.when(giver)
        def _():
            for p in range(PIECES):
                lead(p).wait_send()
            lead_part().wait_send()

        @pl.when(far)
        def _():
            whole = (spike_hi[...], spike_lo[...])
            for p in range(PIECES):
                lead(p).wait_recv()
                joint[strip(seat, p), :] = -mul(split(near_spike[p * step:(p + 1) * step, :]), whole)
                to_side(p).start()
                to_twin(p).start()
            for p in range(PIECES):
                to_side(p).wait_recv()
                relay(p).start()
            lead_part().wait_recv()
            part[...] = part[...] - mul(split(near_part[...]), whole)
            for p in range(PIECES):
                to_twin(p).wait_recv()
            for p in range(PIECES):
                relay(p).wait_recv()
            high, low = split(joint[...])
            spike_hi[...] = high
            spike_lo[...] = low
            for p in range(PIECES):
                to_side(p).wait_send()
                to_twin(p).wait_send()
                relay(p).wait_send()

    def rows_of(c):
        return slice(c * rows, (c + 1) * rows)

    def send(c):
        at = rows_of(c)
        return remote(solved.at[at], inflow.at[at], send_sem.at[c], recv_sem.at[c], {"slab": me + 1})

    def skip(c):
        at = rows_of(c)
        return remote(solved.at[at], inflow.at[at], skip_sem.at[c], recv_sem.at[c], {"slab": me + 2})

    def store(c):
        at = rows_of(c)
        return pltpu.make_async_copy(solved.at[at], out_hbm.at[at], store_sem.at[c])

    sends = jnp.logical_not(last)
    skips = later = None
    if paired:
        sends = sends & (odd | (me < JOIN - 1))
        skips = odd & (me >= JOIN - 1) & (me < n - 2)
        later = skips & (me < n - 3)

    @pl.when(first)
    def _():
        seed.wait()

    for c in range(CHUNKS):
        at = rows_of(c)

        @pl.when(jnp.logical_not(first))
        def _():
            send(c).wait_recv()

        high, low = split(inflow[at, :])
        dot = functools.partial(jnp.dot, preferred_element_type=jnp.float32)
        both = dot(jnp.concatenate([high, low], axis=0), spike_hi[...])
        solved[at, :] = part[at, :] - (both[:rows] + both[rows:] + dot(high, spike_lo[...]))

        @pl.when(sends & jnp.logical_not(later) if paired else sends)
        def _():
            send(c).start()

        if paired:
            @pl.when(skips)
            def _():
                skip(c).start()

        store(c).start()
    if paired:
        @pl.when(later)
        def _():
            for c in range(CHUNKS):
                send(c).start()

    for c in range(CHUNKS):
        store(c).wait()

        @pl.when(sends)
        def _():
            send(c).wait_send()

        if paired:
            @pl.when(skips)
            def _():
                skip(c).wait_send()


def solution(mesh):
    n, group = mesh.shape["slab"], mesh.shape["rhs"]

    def local(diag_blocks, sub_blocks, right_side, boundary):
        width = diag_blocks.shape[1]
        columns = right_side.shape[0]
        square, flat = (width, width), (columns, width)
        f32, bf16 = jnp.float32, jnp.bfloat16
        return pl.pallas_call(
            functools.partial(kernel, n, group),
            out_shape=jax.ShapeDtypeStruct(right_side.shape, f32),
            in_specs=[pl.BlockSpec(memory_space=pl.ANY)] * 4,
            out_specs=pl.BlockSpec(memory_space=pl.ANY),
            scratch_shapes=[
                pltpu.VMEM(square, f32), pltpu.VMEM(square, f32), pltpu.VMEM(flat, f32),
                pltpu.VMEM(square, f32), pltpu.VMEM(square, f32), pltpu.VMEM(square, bf16), pltpu.VMEM(square, bf16),
                pltpu.VMEM(square, bf16), pltpu.VMEM(square, bf16), pltpu.VMEM(square, bf16), pltpu.VMEM(square, bf16),
                pltpu.VMEM(flat, f32), pltpu.VMEM(flat, f32), pltpu.VMEM(flat, f32),
                pltpu.VMEM(square, f32), pltpu.VMEM(flat, f32), pltpu.VMEM((width // group, width), f32), pltpu.VMEM(square, f32),
                pltpu.SemaphoreType.DMA((4,)), *[pltpu.SemaphoreType.DMA((CHUNKS,))] * 4,
                *[pltpu.SemaphoreType.DMA((PIECES,))] * 2, pltpu.SemaphoreType.DMA((2,)),
                *[pltpu.SemaphoreType.DMA((PIECES,))] * 6,
            ],
            compiler_params=pltpu.CompilerParams(collective_id=0, has_side_effects=True),
        )(diag_blocks, sub_blocks, right_side, boundary.T)

    in_specs = (P("slab", None, None), P("slab", None, None), P("rhs", "slab"), P(None, "rhs"))
    return jax.shard_map(local, mesh=mesh, in_specs=in_specs, out_specs=P("rhs", "slab"), check_vma=False)
```
